512 devices in a mesh: list: 32 (over y_hi, x, core), shard: 16 (over z, y_lo).
Axes of the slice: x: 4, y: 8 (y_hi: 4, y_lo: 2; y = y_hi * 2 + y_lo), z: 8, core: 2. Of those that a mesh axis runs over, the one named last changes fastest.
Arguments:
- features: bfloat16 [4096, 4096], P(('list', 'shard')), may hold values from -6 to 6
- norm_gain: float32 [4096], replicated, may hold values from 0.5 to 1.5
- gate_weight: bfloat16 [4096, 11008], P('shard', 'list'), may hold values from -0.09375 to 0.09375
- up_weight: bfloat16 [4096, 11008], P('shard', 'list'), may hold values from -0.09375 to 0.09375
- down_weight: bfloat16 [11008, 4096], P('list', 'shard'), may hold values from -0.0546875 to 0.0546875
- centroids: float32 [64, 4096], P('list'), may hold values from -6 to 6
- list_ids: int32 [4096], P(('list', 'shard')), may hold values from 0 to 63
- live: int32 [4096], P(('list', 'shard')), may hold values 0 or 1
Outputs:
- residuals: bfloat16 [4096, 4096], P(('list', 'shard'))
- refreshed: float32 [64, 4096], P('list')
The draws below stay inside these ranges and needn't reach their ends.
All inputs are finite; a program needn't handle non-finite values. No bound on the sum of `live` on one device may be relied on, other than what follows from the above.
Results may differ from the reference program's by a relative error of at most 0.015.
Values may be sent and summed in bfloat16 or wider, within the bound.
No kernel may reach another device: no remote copies, remote signals or barrier semaphores. Data moves between devices by JAX's collectives and lax.ppermute only.
A program may use at most 64 MiB of HBM per device.

```python
import math
import jax
import jax.numpy as jnp
import numpy as np
from jax import lax

D = 4096
FF = 11008
PASSAGES = 4096
LISTS = 64
N_LIST = 32


def with_ends(drawn, stream_key, low, high):
    shape = drawn.shape
    spot = [jax.random.randint(jax.random.fold_in(stream_key, axis), (), 0, shape[axis]) for axis in range(len(shape))]
    drawn = drawn.at[tuple(spot)].set(low)
    longest = shape.index(max(shape))
    spot[longest] = (spot[longest] + 1) % shape[longest]
    return drawn.at[tuple(spot)].set(high)


def block_levels(rng, extent, shards, smallest, largest):
    loudness = 1.0
    for position, parts in shards:
        heights = jax.random.uniform(jax.random.fold_in(jax.random.fold_in(rng, 6), position), (parts,), jnp.float32, smallest / len(shards), largest / len(shards))
        loudness = loudness * jnp.repeat(jnp.exp(heights), extent[position] // parts).reshape((-1,) + (1,) * (len(extent) - 1 - position))
    return loudness


def rank_bounds(number_of, slope):
    weights = [(1 << 20) // math.isqrt(standing ** slope) + 1 for standing in range(1, number_of + 1)]
    scale = 1 + sum(weights) // (1 << 30)
    return np.cumsum(np.array([max(1, weight // scale) for weight in weights]))


def ranked_ids(rng, shape, amount, skew):
    grid = rank_bounds(amount, skew)
    ticket = jax.random.randint(jax.random.fold_in(rng, 1), shape, 0, int(grid[amount - 1]))
    grade = jnp.searchsorted(jnp.asarray(grid, jnp.int32), ticket, side="right")
    return jax.random.permutation(jax.random.fold_in(rng, 2), amount)[grade].astype(jnp.int32)


def centred(own_key, shape, deviation, limit, split=(), dtype=jnp.bfloat16):
    gain = block_levels(own_key, shape, split, -0.22, 0.18) if split else 1.0
    array = jax.random.normal(own_key, shape, jnp.float32) * deviation * gain
    return jnp.minimum(jnp.maximum(array, -limit), limit).astype(dtype)


def setup_inputs(seed: int = 0) -> dict:
    seeds = jax.random.split(jax.random.key(seed), 9)
    features = centred(seeds[0], (PASSAGES, D), 1.0, 6.0, ((0, 512),))
    norm_gain = jnp.clip(1.0 + 0.1 * jax.random.normal(seeds[1], (D,), jnp.float32), 0.5, 1.5)
    gate_weight = centred(seeds[2], (D, FF), D ** -0.5, 0.09375, ((0, 16), (1, 32)))
    up_weight = centred(seeds[3], (D, FF), D ** -0.5, 0.09375, ((0, 16), (1, 32)))
    down_weight = centred(seeds[4], (FF, D), FF ** -0.5, 0.0546875, ((0, 32), (1, 16)))
    centroids = centred(seeds[5], (LISTS, D), 1.0, 6.0, ((0, 32),), jnp.float32)
    list_ids = with_ends(ranked_ids(seeds[6], (PASSAGES,), LISTS, 2), jax.random.fold_in(seeds[6], 3), 0, LISTS - 1).astype(jnp.int32)
    live = with_ends((jax.random.randint(seeds[7], (PASSAGES,), 0, 8) < 7).astype(jnp.int32), jax.random.fold_in(seeds[7], 1), 0, 1)
    return {"features": features, "norm_gain": norm_gain, "gate_weight": gate_weight, "up_weight": up_weight, "down_weight": down_weight, "centroids": centroids, "list_ids": list_ids, "live": live}


def reference(features, norm_gain, gate_weight, up_weight, down_weight, centroids, list_ids, live):
    gate = jnp.dot(features, gate_weight, preferred_element_type=jnp.float32)
    up_part = jnp.dot(features, up_weight, preferred_element_type=jnp.float32)
    hidden = (jax.nn.silu(gate) * up_part).astype(jnp.bfloat16)
    slice_width = FF // N_LIST
    hidden_parts = hidden.reshape(PASSAGES, N_LIST, slice_width).transpose(1, 0, 2)
    down_parts = down_weight.reshape(N_LIST, slice_width, D)

    def add_term(carry, pair):
        term = jnp.dot(pair[0], pair[1], preferred_element_type=jnp.float32).astype(jnp.bfloat16)
        term = lax.optimization_barrier(term)
        return (carry + term.astype(jnp.float32), None)
    mixed, unused = lax.scan(add_term, jnp.zeros((PASSAGES, D), jnp.float32), (hidden_parts, down_parts))
    stream = features.astype(jnp.float32) + mixed
    scale = lax.rsqrt(lax.optimization_barrier(jnp.mean(stream * stream, axis=1, keepdims=True)) + 1e-05)
    embedding = (stream * scale * norm_gain).astype(jnp.bfloat16)
    rounded = lax.optimization_barrier(centroids.astype(jnp.bfloat16))
    coarse = rounded.astype(jnp.float32)[list_ids]
    alive = live.astype(jnp.float32)
    residuals = (alive[:, None] * (embedding.astype(jnp.float32) - coarse)).astype(jnp.bfloat16)
    sums = jax.ops.segment_sum(embedding.astype(jnp.float32) * alive[:, None], list_ids, num_segments=LISTS)
    counts = jax.ops.segment_sum(alive, list_ids, num_segments=LISTS)
    refreshed = (centroids + sums) / (1.0 + counts[:, None])
    return (residuals, refreshed)
```

```python
import jax
import jax.numpy as jnp
from jax import lax
from jax.sharding import Mesh, PartitionSpec as P

F32 = jnp.float32
BF16 = jnp.bfloat16
SWAP = [(0, 1), (1, 0)]
ROWS = ("yh", "x")
LIST = ("yh", "x", "c")
SHARD = ("z", "yl")


def swapped(value, axis):
    return lax.ppermute(value, axis, SWAP)


def to_everyone(value, axis):
    copies = jnp.broadcast_to(value, (lax.axis_size(axis), *value.shape))
    return lax.all_to_all(copies, axis, split_axis=0, concat_axis=0, tiled=True)


def by_class(value, mine):
    blocks = value.reshape(*value.shape[:-1], 8, 2, 256)
    even = blocks[..., 0, :].reshape(*value.shape[:-1], 2048)
    odd = blocks[..., 1, :].reshape(*value.shape[:-1], 2048)
    return jnp.where(mine == 0, even, odd), jnp.where(mine == 0, odd, even)


def interleaved(own, other, mine):
    even, odd = jnp.where(mine == 0, own, other), jnp.where(mine == 0, other, own)
    shape = own.shape[:-1]
    both = jnp.stack([even.reshape(*shape, 8, 256), odd.reshape(*shape, 8, 256)], axis=-2)
    return both.reshape(*shape, 4096)


def gate_up(rows, weights):
    return jnp.einsum("rzk,zhk->rh", rows, weights, preferred_element_type=F32)


def down(hidden, weights):
    return jnp.einsum("rh,zhk->rzk", hidden, weights, preferred_element_type=F32)


def body(features, norm_gain, gate_weight, up_weight, down_weight, centroids, list_ids, live):
    yl = lax.axis_index("yl")
    first = jnp.concatenate([gate_weight.T, up_weight.T], axis=0)
    first = lax.all_gather(first, "z", axis=0, tiled=False)
    second = lax.all_gather(down_weight, "z", axis=0, tiled=False)

    code = jnp.where(live > 0, list_ids, -1).astype(BF16)
    own_x, away_x = by_class(features, yl)
    code_block = jnp.broadcast_to(code[:, None], (8, 128))
    received = swapped(jnp.concatenate([away_x, code_block], axis=1), "yl")
    x = jnp.concatenate([own_x, received[:, :2048]], axis=0)
    codes = jnp.concatenate([code, received[:, 2048]], axis=0)
    table, _ = by_class(centroids.astype(BF16), yl)
    sent = jnp.concatenate([x, table.reshape(16, 256)], axis=1)
    mine = to_everyone(sent, ROWS)
    theirs = swapped(mine, "c")
    both = jnp.stack([mine, theirs])
    rows = both[..., :2048].reshape(2, 16, 2, 8, 8, 256)
    kept = rows[:, :, 0].reshape(256, 8, 256)
    away = rows[:, :, 1].reshape(256, 8, 256)
    core = lax.axis_index("c")
    lists = both[..., 2048:].reshape(2, 16, 2, 2048)
    lists = jnp.where(core == 0, lists, lists[::-1])
    lists = lists.transpose(1, 0, 2, 3).reshape(64, 2048)

    away_part = gate_up(away, first).astype(BF16)
    away_part = swapped(away_part, "yl")
    whole = gate_up(kept, first) + away_part.astype(F32)
    hidden = (jax.nn.silu(whole[:, :344]) * whole[:, 344:]).astype(BF16)
    other_hidden = swapped(hidden, "yl")
    hidden = jnp.stack([hidden.reshape(2, 128, 344), other_hidden.reshape(2, 128, 344)], axis=1)
    hidden = hidden.reshape(2, 256, 344)
    to_core = down(hidden[1], second).astype(BF16)
    from_core = swapped(to_core, "c")
    terms = (down(hidden[0], second) + from_core.astype(F32)).astype(BF16)
    terms = terms.reshape(2, 16, 8, 2048).transpose(1, 0, 2, 3).reshape(16, 16, 2048)
    terms = lax.all_to_all(terms, ROWS, 0, 0, tiled=True)
    stream = x.astype(F32) + jnp.sum(terms.astype(F32), axis=0)

    square = jnp.sum(stream * stream, axis=1, keepdims=True)
    other_square = swapped(jnp.broadcast_to(square, (16, 128)), "yl")[:, :1]
    other_square = jnp.concatenate([other_square[8:], other_square[:8]], axis=0)
    scale = lax.rsqrt((square + other_square) / 4096.0 + 1e-05)
    gain, _ = by_class(norm_gain, yl)
    embedding = (stream * scale * gain).astype(BF16)

    member = (codes[:, None] == jnp.arange(64, dtype=F32)[None, :].astype(BF16)).astype(BF16)
    alive = (codes >= 0).astype(F32)
    coarse = jnp.dot(member, lists, preferred_element_type=F32)
    residual = (alive[:, None] * (embedding.astype(F32) - coarse)).astype(BF16)
    residuals = interleaved(residual[:8], swapped(residual[8:], "yl"), yl)

    sums = jnp.dot(member.T, embedding, preferred_element_type=F32).astype(BF16)
    counts = jnp.sum(member.astype(F32), axis=0).astype(BF16)
    sums = jnp.concatenate([sums, jnp.broadcast_to(counts[:, None], (64, 128))], axis=1)
    sums = lax.all_to_all(sums.reshape(32, 2, 2176), LIST, 0, 0, tiled=True)
    sums = jnp.sum(sums.astype(F32), axis=0)
    total = to_everyone(sums, SHARD).reshape(8, 2, 2, 2176).sum(axis=0)
    even, odd = total[0], total[1]
    total_counts = even[:, 2048:2049]
    total_sums = jnp.stack(
        [even[:, :2048].reshape(2, 8, 256), odd[:, :2048].reshape(2, 8, 256)], axis=2
    ).reshape(2, 4096)
    refreshed = (centroids + total_sums) / (1.0 + total_counts)
    return residuals, refreshed


def solution(mesh):
    fine = Mesh(mesh.devices.reshape(4, 4, 2, 8, 2), ("yh", "x", "c", "z", "yl"))
    in_specs = (
        P((*LIST, *SHARD), None),
        P(),
        P(SHARD, LIST),
        P(SHARD, LIST),
        P(LIST, SHARD),
        P(LIST, None),
        P((*LIST, *SHARD)),
        P((*LIST, *SHARD)),
    )
    out_specs = (P((*LIST, *SHARD), None), P(LIST, None))
    return jax.shard_map(body, mesh=fine, in_specs=in_specs, out_specs=out_specs, check_vma=False)
```

```python
import jax
import jax.numpy as jnp
from jax import lax
from jax.sharding import Mesh, PartitionSpec as P

F32 = jnp.float32
BF16 = jnp.bfloat16
SWAP = [(0, 1), (1, 0)]
ROWS = ("x", "yh")
LIST = ("yh", "x", "c")
SHARD = ("z", "yl")


def swapped(value, axis):
    return lax.ppermute(value, axis, SWAP)


def to_everyone(value, axis):
    copies = jnp.broadcast_to(value, (lax.axis_size(axis), *value.shape))
    return lax.all_to_all(copies, axis, split_axis=0, concat_axis=0, tiled=True)


def by_class(value, mine):
    blocks = value.reshape(*value.shape[:-1], 8, 2, 256)
    even = blocks[..., 0, :].reshape(*value.shape[:-1], 2048)
    odd = blocks[..., 1, :].reshape(*value.shape[:-1], 2048)
    return jnp.where(mine == 0, even, odd), jnp.where(mine == 0, odd, even)


def interleaved(own, other, mine):
    even, odd = jnp.where(mine == 0, own, other), jnp.where(mine == 0, other, own)
    shape = own.shape[:-1]
    both = jnp.stack([even.reshape(*shape, 8, 256), odd.reshape(*shape, 8, 256)], axis=-2)
    return both.reshape(*shape, 4096)


def gate_up(rows, weights):
    return jnp.einsum("rzk,zhk->rh", rows, weights, preferred_element_type=F32)


def down(hidden, weights):
    return jnp.einsum("rh,zhk->zrk", hidden, weights, preferred_element_type=F32)


def one_hot(codes):
    return (codes[:, None] == jnp.arange(64, dtype=F32)[None, :].astype(BF16)).astype(BF16)


def body(features, norm_gain, gate_weight, up_weight, down_weight, centroids, list_ids, live):
    yl = lax.axis_index("yl")
    weights = jnp.concatenate([gate_weight.T, up_weight.T, down_weight], axis=0)
    weights = lax.all_gather(weights, "z", axis=0, tiled=False)
    first, second = weights[:, :688], weights[:, 688:]

    code = jnp.where(live > 0, list_ids, -1).astype(BF16)
    code_block = jnp.broadcast_to(code[:, None], (8, 128))
    own_x, away_x = by_class(features, yl)
    received = swapped(jnp.concatenate([away_x, code_block], axis=1), "yl")
    x = jnp.concatenate([own_x, received[:, :2048]], axis=0)
    other_code = received[:, 2048]
    table, _ = by_class(centroids.astype(BF16), yl)
    sent = jnp.concatenate([x, table.reshape(16, 256)], axis=1)
    mine = to_everyone(sent, ROWS)
    theirs = swapped(mine, "c")
    both = jnp.stack([mine, theirs])
    rows = both[..., :2048].reshape(2, 16, 2, 8, 8, 256)
    kept = rows[:, :, 0].reshape(256, 8, 256)
    away = rows[:, :, 1].reshape(256, 8, 256)
    core = lax.axis_index("c")
    lists = both[..., 2048:].reshape(2, 4, 4, 2, 2048)
    lists = jnp.where(core == 0, lists, lists[::-1])
    lists = lists.transpose(2, 1, 0, 3, 4).reshape(64, 2048)
    picked = jnp.dot(one_hot(code), lists, preferred_element_type=F32).astype(BF16)
    other_picked = jnp.dot(one_hot(other_code), lists, preferred_element_type=F32).astype(BF16)
    coarse = interleaved(picked, swapped(other_picked, "yl"), yl)

    away_part = gate_up(away, first).astype(BF16)
    away_part = swapped(away_part, "yl")
    whole = gate_up(kept, first) + away_part.astype(F32)
    hidden = (jax.nn.silu(whole[:, :344]) * whole[:, 344:]).astype(BF16)
    other_hidden = swapped(hidden, "yl")
    hidden = jnp.stack([hidden.reshape(2, 4, 32, 344), other_hidden.reshape(2, 4, 32, 344)], axis=2)
    hidden = hidden.reshape(2, 256, 344)
    to_core = down(hidden[1], second).astype(BF16)
    from_core = swapped(to_core, "c")
    terms = (down(hidden[0], second) + from_core.astype(F32)).astype(BF16)
    terms = terms.reshape(8, 4, 64, 256).transpose(1, 0, 2, 3)
    terms = lax.all_to_all(terms, "x", 0, 0, tiled=True)
    terms = jnp.sum(terms.astype(F32), axis=0).astype(BF16)
    terms = terms.reshape(8, 2, 4, 8, 256).transpose(2, 1, 0, 3, 4)
    terms = jnp.where(yl == 0, terms, terms[:, ::-1]).reshape(8, 8, 8, 256)
    terms = lax.all_to_all(terms, ("yh", "yl"), 0, 0, tiled=True)
    terms = jnp.sum(terms.reshape(4, 2, 8, 8, 256).astype(F32), axis=0)
    mixed = terms.transpose(2, 1, 0, 3).reshape(8, 4096)

    stream = features.astype(F32) + mixed
    scale = lax.rsqrt(jnp.mean(stream * stream, axis=1, keepdims=True) + 1e-05)
    embedding = (stream * scale * norm_gain).astype(BF16)
    alive = (live > 0).astype(F32)[:, None]
    residuals = (alive * (embedding.astype(F32) - coarse.astype(F32))).astype(BF16)

    blocks = embedding.reshape(8, 16, 256).transpose(1, 0, 2)
    blocks = jnp.concatenate([blocks, jnp.broadcast_to(code_block, (16, 8, 128))], axis=2)
    blocks = lax.all_to_all(blocks, SHARD, 0, 0, tiled=True).reshape(128, 384)
    member = one_hot(blocks[:, 256])
    sums = jnp.dot(member.T, blocks[:, :256], preferred_element_type=F32).astype(BF16)
    counts = jnp.sum(member.astype(F32), axis=0).astype(BF16)
    sums = jnp.concatenate([sums, jnp.broadcast_to(counts[:, None], (64, 128))], axis=1)
    sums = lax.all_to_all(sums.reshape(32, 2, 384), LIST, 0, 0, tiled=True)
    sums = jnp.sum(sums.astype(F32), axis=0)
    total = to_everyone(sums[:, :256], SHARD).transpose(1, 0, 2).reshape(2, 4096)
    refreshed = (centroids + total) / (1.0 + sums[:, 256:257])
    return residuals, refreshed


def solution(mesh):
    fine = Mesh(mesh.devices.reshape(4, 4, 2, 8, 2), ("yh", "x", "c", "z", "yl"))
    in_specs = (
        P((*LIST, *SHARD), None),
        P(),
        P(SHARD, LIST),
        P(SHARD, LIST),
        P(LIST, SHARD),
        P(LIST, None),
        P((*LIST, *SHARD)),
        P((*LIST, *SHARD)),
    )
    out_specs = (P((*LIST, *SHARD), None), P(LIST, None))
    return jax.shard_map(body, mesh=fine, in_specs=in_specs, out_specs=out_specs, check_vma=False)
```

```python
import jax
import jax.numpy as jnp
from jax import lax
from jax.sharding import Mesh, PartitionSpec as P

F32 = jnp.float32
BF16 = jnp.bfloat16
SWAP = [(0, 1), (1, 0)]
ROWS = ("x", "yh")
LIST = ("yh", "x", "c")
SHARD = ("z", "yl")


def swapped(value, axis):
    return lax.ppermute(value, axis, SWAP)


def to_everyone(value, axis):
    copies = jnp.broadcast_to(value, (lax.axis_size(axis), *value.shape))
    return lax.all_to_all(copies, axis, split_axis=0, concat_axis=0, tiled=True)


def by_class(value, mine):
    blocks = value.reshape(*value.shape[:-1], 8, 2, 256)
    even = blocks[..., 0, :].reshape(*value.shape[:-1], 2048)
    odd = blocks[..., 1, :].reshape(*value.shape[:-1], 2048)
    return jnp.where(mine == 0, even, odd), jnp.where(mine == 0, odd, even)


def interleaved(own, other, mine):
    even, odd = jnp.where(mine == 0, own, other), jnp.where(mine == 0, other, own)
    shape = own.shape[:-1]
    both = jnp.stack([even.reshape(*shape, 8, 256), odd.reshape(*shape, 8, 256)], axis=-2)
    return both.reshape(*shape, 4096)


def gate_up(rows, weights):
    total = 0.0
    for j in (0, 1, 7, 2, 6, 3, 5, 4):
        total += jnp.einsum("rk,hk->rh", rows[:, j], weights[j], preferred_element_type=F32)
    return total


def down(hidden, weights):
    return jnp.einsum("rh,zhk->zrk", hidden, weights, preferred_element_type=F32)


def around(value, axis, index):
    turned = jnp.flip(value, axis)
    return lax.dynamic_slice_in_dim(jnp.concatenate([turned, turned], axis), 7 - index, 8, axis)


def ring(block):
    ahead = [(i, (i + 1) % 8) for i in range(8)]
    back = [(i, (i + 7) % 8) for i in range(8)]
    blocks = [block] + [None] * 7
    up = low = block
    for step in range(1, 4):
        up, low = lax.ppermute(up, "z", ahead), lax.ppermute(low, "z", back)
        blocks[step], blocks[8 - step] = up, low
    halves = lax.ppermute(up[:512], "z", ahead), lax.ppermute(low[512:], "z", back)
    blocks[4] = jnp.concatenate(halves, axis=0)
    return blocks


def one_hot(codes):
    return (codes[:, None] == jnp.arange(64, dtype=F32)[None, :].astype(BF16)).astype(BF16)


def body(features, norm_gain, gate_weight, up_weight, down_weight, centroids, list_ids, live):
    yl = lax.axis_index("yl")
    weights = jnp.concatenate([gate_weight.T, up_weight.T, down_weight], axis=0)
    z = lax.axis_index("z")
    weights = ring(weights)
    first = [w[:688] for w in weights]
    second = jnp.stack([w[688:] for w in weights])

    code = jnp.where(live > 0, list_ids, -1).astype(BF16)
    code_block = jnp.broadcast_to(code[:, None], (8, 128))
    own_x, away_x = (around(v.reshape(8, 8, 256), 1, z).reshape(8, 2048) for v in by_class(features, yl))
    received = swapped(jnp.concatenate([away_x, code_block], axis=1), "yl")
    x = jnp.concatenate([own_x, received[:, :2048]], axis=0)
    other_code = received[:, 2048]
    table, _ = by_class(centroids.astype(BF16), yl)
    sent = jnp.concatenate([x, table.reshape(16, 256)], axis=1)
    mine = to_everyone(to_everyone(sent, "yh"), "x").reshape(16, 16, 2304)
    theirs = swapped(mine, "c")
    both = jnp.stack([mine, theirs])
    rows = both[..., :2048].reshape(2, 16, 2, 8, 8, 256)
    kept = rows[:, :, 0].reshape(256, 8, 256)
    away = rows[:, :, 1].reshape(256, 8, 256)
    core = lax.axis_index("c")
    lists = both[..., 2048:].reshape(2, 4, 4, 2, 2048)
    lists = jnp.where(core == 0, lists, lists[::-1])
    lists = lists.transpose(2, 1, 0, 3, 4).reshape(64, 2048)
    picked = jnp.dot(one_hot(code), lists, preferred_element_type=F32).astype(BF16)
    other_picked = jnp.dot(one_hot(other_code), lists, preferred_element_type=F32).astype(BF16)
    coarse = interleaved(picked, swapped(other_picked, "yl"), yl)

    away_part = gate_up(away, first).astype(BF16)
    away_part = swapped(away_part, "yl")
    whole = gate_up(kept, first) + away_part.astype(F32)
    hidden = (jax.nn.silu(whole[:, :344]) * whole[:, 344:]).astype(BF16)
    other_hidden = swapped(hidden, "yl")
    hidden = jnp.stack([hidden.reshape(2, 4, 32, 344), other_hidden.reshape(2, 4, 32, 344)], axis=2)
    hidden = hidden.reshape(2, 256, 344)
    to_core = down(hidden[1], second).astype(BF16)
    from_core = swapped(to_core, "c")
    terms = (down(hidden[0], second) + from_core.astype(F32)).astype(BF16)
    terms = terms.reshape(8, 4, 64, 256).transpose(1, 0, 2, 3)
    terms = lax.all_to_all(terms, "x", 0, 0, tiled=True)
    terms = jnp.sum(terms.astype(F32), axis=0).astype(BF16)
    terms = terms.reshape(8, 2, 4, 8, 256).transpose(2, 1, 0, 3, 4)
    terms = jnp.where(yl == 0, terms, terms[:, ::-1]).reshape(8, 8, 8, 256)
    terms = lax.all_to_all(terms, ("yh", "yl"), 0, 0, tiled=True)
    terms = jnp.sum(terms.reshape(4, 2, 8, 8, 256).astype(F32), axis=0)
    mixed = around(terms, 1, z).transpose(2, 1, 0, 3).reshape(8, 4096)

    stream = features.astype(F32) + mixed
    scale = lax.rsqrt(jnp.mean(stream * stream, axis=1, keepdims=True) + 1e-05)
    embedding = (stream * scale * norm_gain).astype(BF16)
    alive = (live > 0).astype(F32)[:, None]
    residuals = (alive * (embedding.astype(F32) - coarse.astype(F32))).astype(BF16)

    blocks = embedding.reshape(8, 16, 256).transpose(1, 0, 2)
    blocks = jnp.concatenate([blocks, jnp.broadcast_to(code_block, (16, 8, 128))], axis=2)
    blocks = lax.all_to_all(blocks, SHARD, 0, 0, tiled=True).reshape(128, 384)
    member = one_hot(blocks[:, 256])
    sums = jnp.dot(member.T, blocks[:, :256], preferred_element_type=F32).astype(BF16)
    counts = jnp.sum(member.astype(F32), axis=0).astype(BF16)
    sums = jnp.concatenate([sums, jnp.broadcast_to(counts[:, None], (64, 128))], axis=1)
    sums = lax.all_to_all(sums.reshape(32, 2, 384), LIST, 0, 0, tiled=True)
    sums = jnp.sum(sums.astype(F32), axis=0)
    total = to_everyone(sums[:, :256], SHARD).transpose(1, 0, 2).reshape(2, 4096)
    refreshed = (centroids + total) / (1.0 + sums[:, 256:257])
    return residuals, refreshed


def solution(mesh):
    fine = Mesh(mesh.devices.reshape(4, 4, 2, 8, 2), ("yh", "x", "c", "z", "yl"))
    in_specs = (
        P((*LIST, *SHARD), None),
        P(),
        P(SHARD, LIST),
        P(SHARD, LIST),
        P(LIST, SHARD),
        P(LIST, None),
        P((*LIST, *SHARD)),
        P((*LIST, *SHARD)),
    )
    out_specs = (P((*LIST, *SHARD), None), P(LIST, None))
    return jax.shard_map(body, mesh=fine, in_specs=in_specs, out_specs=out_specs, check_vma=False)
```

```python
import jax
import jax.numpy as jnp
from jax import lax
from jax.experimental import pallas as pl
from jax.experimental.pallas import tpu as pltpu
from jax.sharding import Mesh, PartitionSpec as P

F32 = jnp.float32
BF16 = jnp.bfloat16
SWAP = [(0, 1), (1, 0)]
ROWS = ("x", "yh")
LIST = ("yh", "x", "c")
SHARD = ("z", "yl")


def swapped(value, axis):
    return lax.ppermute(value, axis, SWAP)


def to_everyone(value, axis):
    copies = jnp.broadcast_to(value, (lax.axis_size(axis), *value.shape))
    return lax.all_to_all(copies, axis, split_axis=0, concat_axis=0, tiled=True)


def by_class(value, mine):
    blocks = value.reshape(*value.shape[:-1], 8, 2, 256)
    even = blocks[..., 0, :].reshape(*value.shape[:-1], 2048)
    odd = blocks[..., 1, :].reshape(*value.shape[:-1], 2048)
    return jnp.where(mine == 0, even, odd), jnp.where(mine == 0, odd, even)


def interleaved(own, other, mine):
    even, odd = jnp.where(mine == 0, own, other), jnp.where(mine == 0, other, own)
    shape = own.shape[:-1]
    both = jnp.stack([even.reshape(*shape, 8, 256), odd.reshape(*shape, 8, 256)], axis=-2)
    return both.reshape(*shape, 4096)


def around(value, axis, index):
    turned = jnp.flip(value, axis)
    return lax.dynamic_slice_in_dim(jnp.concatenate([turned, turned], axis), 7 - index, 8, axis)


def ring(block):
    ahead = [(i, (i + 1) % 8) for i in range(8)]
    back = [(i, (i + 7) % 8) for i in range(8)]
    blocks = [block] + [None] * 7
    up = low = block
    for step in range(1, 4):
        up = lax.ppermute(up, "z", ahead)
        low = lax.ppermute(low, "z", back)
        blocks[step], blocks[8 - step] = up, low
    upper = lax.ppermute(up[:512], "z", ahead)
    lower = lax.ppermute(low[512:], "z", back)
    return [*blocks[:4], upper, lower, *blocks[5:]]


def gate_up_kernel(rows, *refs):
    *blocks, upper, lower, out = refs
    for start in range(0, 256, 128):
        total, left, right = 0.0, None, None
        for j in range(8):
            x = rows[start : start + 128, 256 * j : 256 * j + 256]
            if j == 4:
                left, right = times(x, upper[...]), times(x, lower[:176])
            else:
                total += times(x, blocks[j - (j > 4)][:688])
        out[start : start + 128, :512] = (total[:, :512] + left).astype(out.dtype)
        out[start : start + 128, 512:] = (total[:, 512:] + right).astype(out.dtype)


def times(a, b):
    return lax.dot_general(a, b, (((1,), (1,)), ((), ())), preferred_element_type=F32)


VMEM = pl.BlockSpec(memory_space=pltpu.VMEM)


def gate_up(rows, ring_blocks, dtype):
    upper, lower = ring_blocks[4:6]
    blocks = [*ring_blocks[:4], *ring_blocks[6:]]
    return pl.pallas_call(
        gate_up_kernel,
        out_shape=jax.ShapeDtypeStruct((256, 688), dtype),
        in_specs=[VMEM] * 10,
        out_specs=VMEM,
        cost_estimate=pl.CostEstimate(flops=2 * 256 * 2048 * 688, bytes_accessed=4 << 20, transcendentals=0),
        compiler_params=pltpu.CompilerParams(vmem_limit_bytes=16 << 20),
        name="gate_up",
    )(rows, *blocks, upper, lower)


def down_kernel(hidden, *refs):
    *blocks, lower, out = refs
    for j in range(8):
        weights = lower[176:] if j == 4 else blocks[j - (j > 4)][688:]
        out[j] = jnp.dot(hidden[...], weights, preferred_element_type=F32).astype(BF16)


def down_added_kernel(hidden, added, *refs):
    *blocks, lower, out = refs
    for j in range(8):
        weights = lower[176:] if j == 4 else blocks[j - (j > 4)][688:]
        terms = jnp.dot(hidden[...], weights, preferred_element_type=F32)
        terms = (terms + added[j].astype(F32)).astype(BF16)
        for x in range(4):
            out[x, j] = terms[64 * x : 64 * x + 64]


def down(hidden, ring_blocks, added=None):
    blocks = [*ring_blocks[:4], *ring_blocks[6:]]
    shape = (8, 256, 256) if added is None else (4, 8, 64, 256)
    extra = () if added is None else (added,)
    return pl.pallas_call(
        down_kernel if added is None else down_added_kernel,
        out_shape=jax.ShapeDtypeStruct(shape, BF16),
        in_specs=[VMEM] * (9 + len(extra)),
        out_specs=VMEM,
        cost_estimate=pl.CostEstimate(flops=2 * 256 * 2048 * 344, bytes_accessed=3 << 20, transcendentals=0),
        compiler_params=pltpu.CompilerParams(vmem_limit_bytes=16 << 20),
        name="down" if added is None else "down_added",
    )(hidden, *extra, *blocks, ring_blocks[5])


def one_hot(codes):
    return (codes[:, None] == jnp.arange(64, dtype=F32)[None, :].astype(BF16)).astype(BF16)


def program(features, norm_gain, gate_weight, up_weight, down_weight, centroids, list_ids, live):
    yl = lax.axis_index("yl")
    weights = jnp.concatenate([gate_weight.T, up_weight.T, down_weight], axis=0)
    z = lax.axis_index("z")
    weights = ring(weights)

    code = jnp.where(live > 0, list_ids, -1).astype(BF16)
    code_block = jnp.broadcast_to(code[:, None], (8, 128))
    own_x, away_x = (around(v.reshape(8, 8, 256), 1, z).reshape(8, 2048) for v in by_class(features, yl))
    received = swapped(jnp.concatenate([away_x, code_block], axis=1), "yl")
    x = jnp.concatenate([own_x, received[:, :2048]], axis=0)
    other_code = received[:, 2048]
    table, _ = by_class(centroids.astype(BF16), yl)
    sent = jnp.concatenate([x, table.reshape(16, 256)], axis=1)
    mine = to_everyone(sent, ROWS)
    theirs = swapped(mine, "c")
    both = jnp.stack([mine, theirs])
    rows = both[..., :2048].reshape(2, 16, 2, 8, 2048)
    kept = rows[:, :, 0].reshape(256, 2048)
    away = rows[:, :, 1].reshape(256, 2048)
    core = lax.axis_index("c")
    lists = both[..., 2048:].reshape(2, 4, 4, 2, 2048)
    lists = jnp.where(core == 0, lists, lists[::-1])
    lists = lists.transpose(2, 1, 0, 3, 4).reshape(64, 2048)
    picked = jnp.dot(one_hot(code), lists, preferred_element_type=F32).astype(BF16)
    other_picked = jnp.dot(one_hot(other_code), lists, preferred_element_type=F32).astype(BF16)
    coarse = interleaved(picked, swapped(other_picked, "yl"), yl)

    away_part = swapped(gate_up(away, weights, BF16), "yl")
    both = gate_up(kept, weights, F32) + away_part.astype(F32)
    hidden = (jax.nn.silu(both[:, :344]) * both[:, 344:]).astype(BF16)
    other_hidden = swapped(hidden, "yl")
    hidden = jnp.stack([hidden.reshape(2, 4, 32, 344), other_hidden.reshape(2, 4, 32, 344)], axis=2)
    hidden = hidden.reshape(2, 256, 344)
    from_core = swapped(down(hidden[1], weights), "c")
    terms = down(hidden[0], weights, from_core)
    terms = lax.all_to_all(terms, "x", 0, 0, tiled=True)
    terms = jnp.sum(terms.astype(F32), axis=0).astype(BF16)
    terms = terms.reshape(8, 2, 4, 8, 256).transpose(2, 1, 0, 3, 4)
    terms = jnp.where(yl == 0, terms, terms[:, ::-1]).reshape(8, 8, 8, 256)
    terms = lax.all_to_all(terms, ("yh", "yl"), 0, 0, tiled=True)
    terms = jnp.sum(terms.reshape(4, 2, 8, 8, 256).astype(F32), axis=0)
    mixed = around(terms, 1, z).transpose(2, 1, 0, 3).reshape(8, 4096)

    stream = features.astype(F32) + mixed
    scale = lax.rsqrt(jnp.mean(stream * stream, axis=1, keepdims=True) + 1e-05)
    embedding = (stream * scale * norm_gain).astype(BF16)
    alive = (live > 0).astype(F32)[:, None]
    residuals = (alive * (embedding.astype(F32) - coarse.astype(F32))).astype(BF16)

    blocks = embedding.reshape(8, 16, 256).transpose(1, 0, 2)
    blocks = jnp.concatenate([blocks, jnp.broadcast_to(code_block, (16, 8, 128))], axis=2)
    blocks = lax.all_to_all(blocks, SHARD, 0, 0, tiled=True).reshape(128, 384)
    member = one_hot(blocks[:, 256])
    sums = jnp.dot(member.T, blocks[:, :256], preferred_element_type=F32).astype(BF16)
    counts = jnp.sum(member.astype(F32), axis=0).astype(BF16)
    sums = jnp.concatenate([sums, jnp.broadcast_to(counts[:, None], (64, 128))], axis=1)
    sums = lax.all_to_all(sums.reshape(32, 2, 384), LIST, 0, 0, tiled=True)
    sums = jnp.sum(sums.astype(F32), axis=0)
    total = to_everyone(sums[:, :256], SHARD).transpose(1, 0, 2).reshape(2, 4096)
    refreshed = (centroids + total) / (1.0 + sums[:, 256:257])
    return residuals, refreshed


def solution(mesh):
    fine = Mesh(mesh.devices.reshape(4, 4, 2, 8, 2), ("yh", "x", "c", "z", "yl"))
    in_specs = (
        P((*LIST, *SHARD), None),
        P(),
        P(SHARD, LIST),
        P(SHARD, LIST),
        P(LIST, SHARD),
        P(LIST, None),
        P((*LIST, *SHARD)),
        P((*LIST, *SHARD)),
    )
    out_specs = (P((*LIST, *SHARD), None), P(LIST, None))
    return jax.shard_map(program, mesh=fine, in_specs=in_specs, out_specs=out_specs, check_vma=False)
```

```python
import jax
import jax.numpy as jnp
from jax import lax
from jax.experimental import pallas as pl
from jax.experimental.pallas import tpu as pltpu
from jax.sharding import Mesh, PartitionSpec as P

F32 = jnp.float32
BF16 = jnp.bfloat16
SWAP = [(0, 1), (1, 0)]
ROWS = ("x", "yh")
LIST = ("yh", "x", "c")
SHARD = ("z", "yl")


def swapped(value, axis):
    return lax.ppermute(value, axis, SWAP)


def to_everyone(value, axis):
    copies = jnp.broadcast_to(value, (lax.axis_size(axis), *value.shape))
    return lax.all_to_all(copies, axis, split_axis=0, concat_axis=0, tiled=True)


def by_class(value, mine):
    blocks = value.reshape(*value.shape[:-1], 8, 2, 256)
    even = blocks[..., 0, :].reshape(*value.shape[:-1], 2048)
    odd = blocks[..., 1, :].reshape(*value.shape[:-1], 2048)
    return jnp.where(mine == 0, even, odd), jnp.where(mine == 0, odd, even)


def interleaved(own, other, mine):
    even, odd = jnp.where(mine == 0, own, other), jnp.where(mine == 0, other, own)
    shape = own.shape[:-1]
    both = jnp.stack([even.reshape(*shape, 8, 256), odd.reshape(*shape, 8, 256)], axis=-2)
    return both.reshape(*shape, 4096)


def around(value, axis, index):
    turned = jnp.flip(value, axis)
    return lax.dynamic_slice_in_dim(jnp.concatenate([turned, turned], axis), 7 - index, 8, axis)


AHEAD = [(i, (i + 1) % 8) for i in range(8)]
BACK = [(i, (i + 7) % 8) for i in range(8)]


def hop(value, pairs):
    return lax.ppermute(value, "z", pairs)


def rings(first, second):
    firsts, seconds = [first] + [None] * 7, [second] + [None] * 7
    for step in range(1, 4):
        firsts[step] = hop(firsts[step - 1], AHEAD)
        firsts[8 - step] = hop(firsts[(9 - step) % 8], BACK)
        seconds[step] = hop(seconds[step - 1], AHEAD)
        seconds[8 - step] = hop(seconds[(9 - step) % 8], BACK)
    upper = hop(firsts[3][:384], AHEAD)
    lower = hop(firsts[5][384:], BACK)
    seconds[4] = hop(seconds[3], AHEAD)
    return [*firsts[:4], *firsts[5:], upper, lower], seconds


def gate_up_kernel(rows, *refs):
    *blocks, upper, lower, out = refs
    for start in range(0, 256, 128):
        total = 0.0
        for j in (0, 1, 2, 3, 5, 6, 7):
            x = rows[start : start + 128, 256 * j : 256 * j + 256]
            total += times(x, blocks[j - (j > 4)][...])
        x = rows[start : start + 128, 1024:1280]
        out[start : start + 128, :384] = (total[:, :384] + times(x, upper[...])).astype(out.dtype)
        out[start : start + 128, 384:] = (total[:, 384:] + times(x, lower[...])).astype(out.dtype)


def times(a, b):
    return lax.dot_general(a, b, (((1,), (1,)), ((), ())), preferred_element_type=F32)


VMEM = pl.BlockSpec(memory_space=pltpu.VMEM)


def whole(shape):
    return pl.BlockSpec(shape, lambda: (0,) * len(shape))


def gate_up(rows, blocks, dtype):
    return pl.pallas_call(
        gate_up_kernel,
        out_shape=jax.ShapeDtypeStruct((256, 688), dtype),
        in_specs=[VMEM] * 10,
        out_specs=VMEM,
        cost_estimate=pl.CostEstimate(flops=2 * 256 * 2048 * 688, bytes_accessed=4 << 20, transcendentals=0),
        compiler_params=pltpu.CompilerParams(vmem_limit_bytes=16 << 20),
        name="gate_up",
    )(rows, *blocks)


def rows_of(core, own, other):
    pieces = []
    for at in range(128 * core, 128 * core + 128, 32):
        pieces += [own[at : at + 32], other[at : at + 32]]
    return jnp.concatenate(pieces, axis=0)


def down_kernel(own, other, *refs):
    *blocks, out = refs
    hidden = rows_of(1, own, other)
    for j in range(8):
        out[j] = jnp.dot(hidden, blocks[j][...], preferred_element_type=F32).astype(BF16)


def down_added_kernel(own, other, added, *refs):
    *blocks, out = refs
    hidden = rows_of(0, own, other)
    for j in range(8):
        terms = jnp.dot(hidden, blocks[j][...], preferred_element_type=F32)
        terms = (terms + added[j].astype(F32)).astype(BF16)
        for x in range(4):
            out[x, j] = terms[64 * x : 64 * x + 64]


def down(own, other, blocks, *added):
    shape = (4, 8, 64, 256) if added else (8, 256, 256)
    return pl.pallas_call(
        down_added_kernel if added else down_kernel,
        out_shape=jax.ShapeDtypeStruct(shape, BF16),
        in_specs=[VMEM] * (10 + len(added)),
        out_specs=whole(shape) if added else VMEM,
        cost_estimate=pl.CostEstimate(flops=2 * 256 * 2048 * 344, bytes_accessed=3 << 20, transcendentals=0),
        compiler_params=pltpu.CompilerParams(vmem_limit_bytes=16 << 20),
        name="down_added" if added else "down",
    )(own, other, *added, *blocks)


def one_hot(codes):
    return (codes[:, None] == jnp.arange(64, dtype=F32)[None, :].astype(BF16)).astype(BF16)


def program(features, norm_gain, gate_weight, up_weight, down_weight, centroids, list_ids, live):
    yl = lax.axis_index("yl")
    z = lax.axis_index("z")
    first, second = rings(jnp.concatenate([gate_weight.T, up_weight.T], axis=0), down_weight)

    code = jnp.where(live > 0, list_ids, -1).astype(BF16)
    code_block = jnp.broadcast_to(code[:, None], (8, 128))
    own_x, away_x = (around(v.reshape(8, 8, 256), 1, z).reshape(8, 2048) for v in by_class(features, yl))
    received = swapped(jnp.concatenate([away_x, code_block], axis=1), "yl")
    x = jnp.concatenate([own_x, received[:, :2048]], axis=0)
    other_code = received[:, 2048]
    table, _ = by_class(centroids.astype(BF16), yl)
    sent = jnp.concatenate([x, table.reshape(16, 256)], axis=1)
    mine = to_everyone(sent, ROWS)
    theirs = swapped(mine, "c")
    both = jnp.stack([mine, theirs])
    rows = both[..., :2048].reshape(2, 16, 2, 8, 2048)
    kept = rows[:, :, 0].reshape(256, 2048)
    away = rows[:, :, 1].reshape(256, 2048)
    away_part = swapped(gate_up(away, first, BF16), "yl")
    both = gate_up(kept, first, F32) + away_part.astype(F32)
    hidden = (jax.nn.silu(both[:, :344]) * both[:, 344:]).astype(BF16)
    other_hidden = swapped(hidden, "yl")
    from_core = swapped(down(hidden, other_hidden, second), "c")
    terms = down(hidden, other_hidden, second, from_core)

    mine, theirs, terms = lax.optimization_barrier((mine, theirs, terms))
    core = lax.axis_index("c")
    lists = jnp.stack([mine[..., 2048:], theirs[..., 2048:]]).reshape(2, 4, 4, 2, 2048)
    lists = jnp.where(core == 0, lists, lists[::-1])
    lists = lists.transpose(2, 1, 0, 3, 4).reshape(64, 2048)
    picked = jnp.dot(one_hot(code), lists, preferred_element_type=F32).astype(BF16)
    other_picked = jnp.dot(one_hot(other_code), lists, preferred_element_type=F32).astype(BF16)
    coarse = interleaved(picked, swapped(other_picked, "yl"), yl)

    terms = lax.all_to_all(terms, "x", 0, 0, tiled=True)
    terms = jnp.sum(terms.astype(F32), axis=0).astype(BF16)
    terms = terms.reshape(8, 2, 4, 8, 256).transpose(2, 1, 0, 3, 4)
    terms = jnp.where(yl == 0, terms, terms[:, ::-1]).reshape(8, 8, 8, 256)
    terms = lax.all_to_all(terms, ("yh", "yl"), 0, 0, tiled=True)
    terms = jnp.sum(terms.reshape(4, 2, 8, 8, 256).astype(F32), axis=0)
    mixed = around(terms, 1, z).transpose(2, 1, 0, 3).reshape(8, 4096)

    stream = features.astype(F32) + mixed
    scale = lax.rsqrt(jnp.mean(stream * stream, axis=1, keepdims=True) + 1e-05)
    embedding = (stream * scale * norm_gain).astype(BF16)
    alive = (live > 0).astype(F32)[:, None]
    residuals = (alive * (embedding.astype(F32) - coarse.astype(F32))).astype(BF16)

    blocks = embedding.reshape(8, 16, 256).transpose(1, 0, 2)
    blocks = jnp.concatenate([blocks, jnp.broadcast_to(code_block, (16, 8, 128))], axis=2)
    blocks = lax.all_to_all(blocks, SHARD, 0, 0, tiled=True).reshape(128, 384)
    member = one_hot(blocks[:, 256])
    sums = jnp.dot(member.T, blocks[:, :256], preferred_element_type=F32).astype(BF16)
    counts = jnp.sum(member.astype(F32), axis=0).astype(BF16)
    sums = jnp.concatenate([sums, jnp.broadcast_to(counts[:, None], (64, 128))], axis=1)
    sums = lax.all_to_all(sums.reshape(32, 2, 384), LIST, 0, 0, tiled=True)
    sums = jnp.sum(sums.astype(F32), axis=0)
    total = to_everyone(sums[:, :256], SHARD).transpose(1, 0, 2).reshape(2, 4096)
    refreshed = (centroids + total) / (1.0 + sums[:, 256:257])
    return residuals, refreshed


def solution(mesh):
    fine = Mesh(mesh.devices.reshape(4, 4, 2, 8, 2), ("yh", "x", "c", "z", "yl"))
    in_specs = (
        P((*LIST, *SHARD), None),
        P(),
        P(SHARD, LIST),
        P(SHARD, LIST),
        P(LIST, SHARD),
        P(LIST, None),
        P((*LIST, *SHARD)),
        P((*LIST, *SHARD)),
    )
    out_specs = (P((*LIST, *SHARD), None), P(LIST, None))
    return jax.shard_map(program, mesh=fine, in_specs=in_specs, out_specs=out_specs, check_vma=False)
```

```python
import jax
import jax.numpy as jnp
from jax import lax
from jax.experimental import pallas as pl
from jax.experimental.pallas import tpu as pltpu
from jax.sharding import Mesh, PartitionSpec as P

F32 = jnp.float32
BF16 = jnp.bfloat16
SWAP = [(0, 1), (1, 0)]
ROWS = ("x", "yh")
LIST = ("yh", "x", "c")
SHARD = ("z", "yl")


def swapped(value, axis):
    return lax.ppermute(value, axis, SWAP)


def to_everyone(value, axis):
    copies = jnp.broadcast_to(value, (lax.axis_size(axis), *value.shape))
    return lax.all_to_all(copies, axis, split_axis=0, concat_axis=0, tiled=True)


def by_class(value, mine):
    blocks = value.reshape(*value.shape[:-1], 8, 2, 256)
    even = blocks[..., 0, :].reshape(*value.shape[:-1], 2048)
    odd = blocks[..., 1, :].reshape(*value.shape[:-1], 2048)
    return jnp.where(mine == 0, even, odd), jnp.where(mine == 0, odd, even)


def interleaved(own, other, mine):
    even, odd = jnp.where(mine == 0, own, other), jnp.where(mine == 0, other, own)
    shape = own.shape[:-1]
    both = jnp.stack([even.reshape(*shape, 8, 256), odd.reshape(*shape, 8, 256)], axis=-2)
    return both.reshape(*shape, 4096)


def around(value, axis, index):
    turned = jnp.flip(value, axis)
    return lax.dynamic_slice_in_dim(jnp.concatenate([turned, turned], axis), 7 - index, 8, axis)


AHEAD = [(i, (i + 1) % 8) for i in range(8)]
BACK = [(i, (i + 7) % 8) for i in range(8)]


def hop(value, pairs):
    return lax.ppermute(value, "z", pairs)


def ring(block):
    blocks = [block] + [None] * 7
    for step in range(1, 4):
        blocks[step] = hop(blocks[step - 1], AHEAD)
        blocks[8 - step] = hop(blocks[(9 - step) % 8], BACK)
    blocks[4] = hop(blocks[3], AHEAD)
    return blocks


EARLY = (0, 1, 7, 2, 6, 3, 5)


def early_kernel(rows, *refs):
    *blocks, out = refs
    for start in range(0, 256, 128):
        total = 0.0
        for j, block in zip(EARLY, blocks):
            x = rows[start : start + 128, 256 * j : 256 * j + 256]
            total += times(x, block[:688])
        out[start : start + 128] = total


def last_kernel(rows, early, block, out):
    out[...] = (early[...] + times(rows[:, 1024:1280], block[:688])).astype(out.dtype)


def times(a, b):
    return lax.dot_general(a, b, (((1,), (1,)), ((), ())), preferred_element_type=F32)


VMEM = pl.BlockSpec(memory_space=pltpu.VMEM)


def whole(shape):
    return pl.BlockSpec(shape, lambda: (0,) * len(shape))


def product(kernel, dtype, depth, *operands):
    return pl.pallas_call(
        kernel,
        out_shape=jax.ShapeDtypeStruct((256, 688), dtype),
        in_specs=[VMEM] * len(operands),
        out_specs=VMEM,
        cost_estimate=pl.CostEstimate(flops=2 * 256 * depth * 688, bytes_accessed=2048 * depth, transcendentals=0),
        compiler_params=pltpu.CompilerParams(vmem_limit_bytes=16 << 20),
    )(*operands)


def early_product(rows, blocks):
    return product(early_kernel, F32, 1792, rows, *[blocks[j] for j in EARLY])


def last_product(rows, early, blocks, dtype):
    return product(last_kernel, dtype, 256, rows, early, blocks[4])


def rows_of(core, own, other):
    pieces = []
    for at in range(128 * core, 128 * core + 128, 32):
        pieces += [own[at : at + 32], other[at : at + 32]]
    return jnp.concatenate(pieces, axis=0)


def down_kernel(own, other, *refs):
    *blocks, out = refs
    hidden = rows_of(1, own, other)
    for j in range(8):
        out[j] = jnp.dot(hidden, blocks[j][688:], preferred_element_type=F32).astype(BF16)


def down_added_kernel(own, other, added, *refs):
    *blocks, out = refs
    hidden = rows_of(0, own, other)
    for j in range(8):
        terms = jnp.dot(hidden, blocks[j][688:], preferred_element_type=F32)
        terms = (terms + added[j].astype(F32)).astype(BF16)
        for x in range(4):
            out[x, j] = terms[64 * x : 64 * x + 64]


def down(own, other, blocks, *added):
    shape = (4, 8, 64, 256) if added else (8, 256, 256)
    return pl.pallas_call(
        down_added_kernel if added else down_kernel,
        out_shape=jax.ShapeDtypeStruct(shape, BF16),
        in_specs=[VMEM] * (10 + len(added)),
        out_specs=whole(shape) if added else VMEM,
        cost_estimate=pl.CostEstimate(flops=2 * 256 * 2048 * 344, bytes_accessed=3 << 20, transcendentals=0),
        compiler_params=pltpu.CompilerParams(vmem_limit_bytes=16 << 20),
        name="down_added" if added else "down",
    )(own, other, *added, *blocks)


def one_hot(codes):
    return (codes[:, None] == jnp.arange(64, dtype=F32)[None, :].astype(BF16)).astype(BF16)


def program(features, norm_gain, gate_weight, up_weight, down_weight, centroids, list_ids, live):
    yl = lax.axis_index("yl")
    z = lax.axis_index("z")
    weights = ring(jnp.concatenate([gate_weight.T, up_weight.T, down_weight], axis=0))

    code = jnp.where(live > 0, list_ids, -1).astype(BF16)
    code_block = jnp.broadcast_to(code[:, None], (8, 128))
    own_x, away_x = (around(v.reshape(8, 8, 256), 1, z).reshape(8, 2048) for v in by_class(features, yl))
    received = swapped(jnp.concatenate([away_x, code_block], axis=1), "yl")
    x = jnp.concatenate([own_x, received[:, :2048]], axis=0)
    other_code = received[:, 2048]
    table, _ = by_class(centroids.astype(BF16), yl)
    sent = jnp.concatenate([x, table.reshape(16, 256)], axis=1)
    mine = to_everyone(sent, ROWS)
    theirs = swapped(mine, "c")
    both = jnp.stack([mine, theirs])
    rows = both[..., :2048].reshape(2, 16, 2, 8, 2048)
    kept = rows[:, :, 0].reshape(256, 2048)
    away = rows[:, :, 1].reshape(256, 2048)
    away_early, kept_early = early_product(away, weights), early_product(kept, weights)
    away_part = swapped(last_product(away, away_early, weights, BF16), "yl")
    both = last_product(kept, kept_early, weights, F32) + away_part.astype(F32)
    hidden = (jax.nn.silu(both[:, :344]) * both[:, 344:]).astype(BF16)
    other_hidden = swapped(hidden, "yl")
    from_core = swapped(down(hidden, other_hidden, weights), "c")
    terms = down(hidden, other_hidden, weights, from_core)

    mine, theirs, terms = lax.optimization_barrier((mine, theirs, terms))
    core = lax.axis_index("c")
    lists = jnp.stack([mine[..., 2048:], theirs[..., 2048:]]).reshape(2, 4, 4, 2, 2048)
    lists = jnp.where(core == 0, lists, lists[::-1])
    lists = lists.transpose(2, 1, 0, 3, 4).reshape(64, 2048)
    picked = jnp.dot(one_hot(code), lists, preferred_element_type=F32).astype(BF16)
    other_picked = jnp.dot(one_hot(other_code), lists, preferred_element_type=F32).astype(BF16)
    coarse = interleaved(picked, swapped(other_picked, "yl"), yl)

    terms = lax.all_to_all(terms, "x", 0, 0, tiled=True)
    terms = jnp.sum(terms.astype(F32), axis=0).astype(BF16)
    terms = terms.reshape(8, 2, 4, 8, 256).transpose(2, 1, 0, 3, 4)
    terms = jnp.where(yl == 0, terms, terms[:, ::-1]).reshape(8, 8, 8, 256)
    terms = lax.all_to_all(terms, ("yh", "yl"), 0, 0, tiled=True)
    terms = jnp.sum(terms.reshape(4, 2, 8, 8, 256).astype(F32), axis=0)
    mixed = around(terms, 1, z).transpose(2, 1, 0, 3).reshape(8, 4096)

    stream = features.astype(F32) + mixed
    scale = lax.rsqrt(jnp.mean(stream * stream, axis=1, keepdims=True) + 1e-05)
    embedding = (stream * scale * norm_gain).astype(BF16)
    alive = (live > 0).astype(F32)[:, None]
    residuals = (alive * (embedding.astype(F32) - coarse.astype(F32))).astype(BF16)

    blocks = embedding.reshape(8, 16, 256).transpose(1, 0, 2)
    blocks = jnp.concatenate([blocks, jnp.broadcast_to(code_block, (16, 8, 128))], axis=2)
    blocks = lax.all_to_all(blocks, SHARD, 0, 0, tiled=True).reshape(128, 384)
    member = one_hot(blocks[:, 256])
    sums = jnp.dot(member.T, blocks[:, :256], preferred_element_type=F32).astype(BF16)
    counts = jnp.sum(member.astype(F32), axis=0).astype(BF16)
    sums = jnp.concatenate([sums, jnp.broadcast_to(counts[:, None], (64, 128))], axis=1)
    sums = lax.all_to_all(sums.reshape(32, 2, 384), LIST, 0, 0, tiled=True)
    sums = jnp.sum(sums.astype(F32), axis=0)
    total = to_everyone(sums[:, :256], SHARD).transpose(1, 0, 2).reshape(2, 4096)
    refreshed = (centroids + total) / (1.0 + sums[:, 256:257])
    return residuals, refreshed


def solution(mesh):
    fine = Mesh(mesh.devices.reshape(4, 4, 2, 8, 2), ("yh", "x", "c", "z", "yl"))
    in_specs = (
        P((*LIST, *SHARD), None),
        P(),
        P(SHARD, LIST),
        P(SHARD, LIST),
        P(LIST, SHARD),
        P(LIST, None),
        P((*LIST, *SHARD)),
        P((*LIST, *SHARD)),
    )
    out_specs = (P((*LIST, *SHARD), None), P(LIST, None))
    return jax.shard_map(program, mesh=fine, in_specs=in_specs, out_specs=out_specs, check_vma=False)
```

```python
import functools

import jax
import jax.numpy as jnp
from jax import lax
from jax.experimental import pallas as pl
from jax.experimental.pallas import tpu as pltpu
from jax.sharding import Mesh, PartitionSpec as P

F32 = jnp.float32
BF16 = jnp.bfloat16
SWAP = [(0, 1), (1, 0)]
ROWS = ("x", "yh")
LIST = ("yh", "x", "c")
SHARD = ("z", "yl")


def swapped(value, axis):
    return lax.ppermute(value, axis, SWAP)


def to_everyone(value, axis):
    copies = jnp.broadcast_to(value, (lax.axis_size(axis), *value.shape))
    return lax.all_to_all(copies, axis, split_axis=0, concat_axis=0, tiled=True)


def by_class(value, mine):
    blocks = value.reshape(*value.shape[:-1], 8, 2, 256)
    even = blocks[..., 0, :].reshape(*value.shape[:-1], 2048)
    odd = blocks[..., 1, :].reshape(*value.shape[:-1], 2048)
    return jnp.where(mine == 0, even, odd), jnp.where(mine == 0, odd, even)


def interleaved(own, other, mine):
    even, odd = jnp.where(mine == 0, own, other), jnp.where(mine == 0, other, own)
    shape = own.shape[:-1]
    both = jnp.stack([even.reshape(*shape, 8, 256), odd.reshape(*shape, 8, 256)], axis=-2)
    return both.reshape(*shape, 4096)


def around(value, axis, index):
    turned = jnp.flip(value, axis)
    return lax.dynamic_slice_in_dim(jnp.concatenate([turned, turned], axis), 7 - index, 8, axis)


AHEAD = [(i, (i + 1) % 8) for i in range(8)]
BACK = [(i, (i + 7) % 8) for i in range(8)]


def hop(value, pairs):
    return lax.ppermute(value, "z", pairs)


def ring(block):
    blocks = [block] + [None] * 7
    for step in range(1, 4):
        blocks[step] = hop(blocks[step - 1], AHEAD)
        blocks[8 - step] = hop(blocks[(9 - step) % 8], BACK)
    fourth = hop(blocks[3][:688], AHEAD), hop(blocks[5][688:], BACK)
    return [*blocks[:4], *blocks[5:]], *fourth


EARLY = (0, 1, 2, 3, 5, 6, 7)


def early_kernel(rows, *refs):
    *blocks, out = refs
    for start in range(0, 256, 128):
        total = 0.0
        for j, block in zip(EARLY, blocks):
            x = rows[start : start + 128, 256 * j : 256 * j + 256]
            total += times(x, block[:688])
        out[start : start + 128] = total


def last_kernel(rows, early, block, out):
    out[...] = (early[...] + times(rows[:, 1024:1280], block[...])).astype(out.dtype)


def times(a, b):
    return lax.dot_general(a, b, (((1,), (1,)), ((), ())), preferred_element_type=F32)


VMEM = pl.BlockSpec(memory_space=pltpu.VMEM)


def product(kernel, dtype, depth, *operands):
    return pl.pallas_call(
        kernel,
        out_shape=jax.ShapeDtypeStruct((256, 688), dtype),
        in_specs=[VMEM] * len(operands),
        out_specs=VMEM,
        cost_estimate=pl.CostEstimate(flops=2 * 256 * depth * 688, bytes_accessed=2048 * depth, transcendentals=0),
        compiler_params=pltpu.CompilerParams(vmem_limit_bytes=16 << 20),
    )(*operands)


def early_product(rows, blocks):
    return product(early_kernel, F32, 1792, rows, *blocks)


def last_product(rows, early, block, dtype):
    return product(last_kernel, dtype, 256, rows, early, block)


def rows_of(core, own, other):
    pieces = []
    for at in range(128 * core, 128 * core + 128, 32):
        pieces += [own[at : at + 32], other[at : at + 32]]
    return jnp.concatenate(pieces, axis=0)


def down_kernel(core, own, other, fourth, *refs):
    *blocks, out = refs
    hidden = rows_of(core, own, other)
    for j in range(8):
        weights = fourth[...] if j == 4 else blocks[j - (j > 4)][688:]
        terms = jnp.dot(hidden, weights, preferred_element_type=F32).astype(out.dtype)
        for x in range(4):
            out[x, j] = terms[64 * x : 64 * x + 64]


def down(core, dtype, own, other, fourth, blocks):
    return pl.pallas_call(
        functools.partial(down_kernel, core),
        out_shape=jax.ShapeDtypeStruct((4, 8, 64, 256), dtype),
        in_specs=[VMEM] * 10,
        out_specs=VMEM,
        cost_estimate=pl.CostEstimate(flops=2 * 256 * 2048 * 344, bytes_accessed=3 << 20, transcendentals=0),
        compiler_params=pltpu.CompilerParams(vmem_limit_bytes=16 << 20),
    )(own, other, fourth, *blocks)


def one_hot(codes):
    return (codes[:, None] == jnp.arange(64, dtype=F32)[None, :].astype(BF16)).astype(BF16)


def program(features, norm_gain, gate_weight, up_weight, down_weight, centroids, list_ids, live):
    yl = lax.axis_index("yl")
    z = lax.axis_index("z")
    weights, last_first, last_second = ring(jnp.concatenate([gate_weight.T, up_weight.T, down_weight], axis=0))

    code = jnp.where(live > 0, list_ids, -1).astype(BF16)
    code_block = jnp.broadcast_to(code[:, None], (8, 128))
    own_x, away_x = (around(v.reshape(8, 8, 256), 1, z).reshape(8, 2048) for v in by_class(features, yl))
    received = swapped(jnp.concatenate([away_x, code_block], axis=1), "yl")
    x = jnp.concatenate([own_x, received[:, :2048]], axis=0)
    other_code = received[:, 2048]
    table, _ = by_class(centroids.astype(BF16), yl)
    sent = jnp.concatenate([x, table.reshape(16, 256)], axis=1)
    mine = to_everyone(sent, ROWS)
    theirs = swapped(mine, "c")
    both = jnp.stack([mine, theirs])
    rows = both[..., :2048].reshape(2, 16, 2, 8, 2048)
    kept = rows[:, :, 0].reshape(256, 2048)
    away = rows[:, :, 1].reshape(256, 2048)
    away_early = early_product(away, weights)
    away_part = last_product(away, away_early, last_first, BF16)
    away_part = swapped(away_part, "yl")
    kept_part = last_product(kept, early_product(kept, weights), last_first, F32)
    both = kept_part + away_part.astype(F32)
    hidden = (jax.nn.silu(both[:, :344]) * both[:, 344:]).astype(BF16)
    other_hidden = swapped(hidden, "yl")
    to_core = down(1, BF16, hidden, other_hidden, last_second, weights)
    from_core = swapped(to_core, "c")
    terms = down(0, F32, hidden, other_hidden, last_second, weights)
    terms = (terms + from_core.astype(F32)).astype(BF16)

    mine, theirs, terms = lax.optimization_barrier((mine, theirs, terms))
    core = lax.axis_index("c")
    lists = jnp.stack([mine[..., 2048:], theirs[..., 2048:]]).reshape(2, 4, 4, 2, 2048)
    lists = jnp.where(core == 0, lists, lists[::-1])
    lists = lists.transpose(2, 1, 0, 3, 4).reshape(64, 2048)
    picked = jnp.dot(one_hot(code), lists, preferred_element_type=F32).astype(BF16)
    other_picked = jnp.dot(one_hot(other_code), lists, preferred_element_type=F32).astype(BF16)
    coarse = interleaved(picked, swapped(other_picked, "yl"), yl)

    terms = lax.all_to_all(terms, "x", 0, 0, tiled=True)
    terms = jnp.sum(terms.astype(F32), axis=0).astype(BF16)
    terms = terms.reshape(8, 2, 4, 8, 256).transpose(2, 1, 0, 3, 4)
    terms = jnp.where(yl == 0, terms, terms[:, ::-1]).reshape(8, 8, 8, 256)
    terms = lax.all_to_all(terms, ("yh", "yl"), 0, 0, tiled=True)
    terms = jnp.sum(terms.reshape(4, 2, 8, 8, 256).astype(F32), axis=0)
    mixed = around(terms, 1, z).transpose(2, 1, 0, 3).reshape(8, 4096)

    stream = features.astype(F32) + mixed
    scale = lax.rsqrt(jnp.mean(stream * stream, axis=1, keepdims=True) + 1e-05)
    embedding = (stream * scale * norm_gain).astype(BF16)
    alive = (live > 0).astype(F32)[:, None]
    residuals = (alive * (embedding.astype(F32) - coarse.astype(F32))).astype(BF16)

    blocks = embedding.reshape(8, 16, 256).transpose(1, 0, 2)
    blocks = jnp.concatenate([blocks, jnp.broadcast_to(code_block, (16, 8, 128))], axis=2)
    blocks = lax.all_to_all(blocks, SHARD, 0, 0, tiled=True).reshape(128, 384)
    member = one_hot(blocks[:, 256])
    sums = jnp.dot(member.T, blocks[:, :256], preferred_element_type=F32).astype(BF16)
    counts = jnp.sum(member.astype(F32), axis=0).astype(BF16)
    sums = jnp.concatenate([sums, jnp.broadcast_to(counts[:, None], (64, 128))], axis=1)
    sums = lax.all_to_all(sums.reshape(32, 2, 384), LIST, 0, 0, tiled=True)
    sums = jnp.sum(sums.astype(F32), axis=0)
    total = to_everyone(sums[:, :256], SHARD).transpose(1, 0, 2).reshape(2, 4096)
    refreshed = (centroids + total) / (1.0 + sums[:, 256:257])
    return residuals, refreshed


def solution(mesh):
    fine = Mesh(mesh.devices.reshape(4, 4, 2, 8, 2), ("yh", "x", "c", "z", "yl"))
    in_specs = (
        P((*LIST, *SHARD), None),
        P(),
        P(SHARD, LIST),
        P(SHARD, LIST),
        P(LIST, SHARD),
        P(LIST, None),
        P((*LIST, *SHARD)),
        P((*LIST, *SHARD)),
    )
    out_specs = (P((*LIST, *SHARD), None), P(LIST, None))
    return jax.shard_map(program, mesh=fine, in_specs=in_specs, out_specs=out_specs, check_vma=False)
```

```python
import functools

import jax
import jax.numpy as jnp
from jax import lax
from jax.experimental import pallas as pl
from jax.experimental.pallas import tpu as pltpu
from jax.sharding import Mesh, PartitionSpec as P

F32 = jnp.float32
BF16 = jnp.bfloat16
SWAP = [(0, 1), (1, 0)]
ROWS = ("x", "yh")
LIST = ("yh", "x", "c")
SHARD = ("z", "yl")


def swapped(value, axis):
    return lax.ppermute(value, axis, SWAP)


def to_everyone(value, axis):
    copies = jnp.broadcast_to(value, (lax.axis_size(axis), *value.shape))
    return lax.all_to_all(copies, axis, split_axis=0, concat_axis=0, tiled=True)


def by_class(value, mine):
    blocks = value.reshape(*value.shape[:-1], 8, 2, 256)
    even = blocks[..., 0, :].reshape(*value.shape[:-1], 2048)
    odd = blocks[..., 1, :].reshape(*value.shape[:-1], 2048)
    return jnp.where(mine == 0, even, odd), jnp.where(mine == 0, odd, even)


def interleaved(own, other, mine):
    even, odd = jnp.where(mine == 0, own, other), jnp.where(mine == 0, other, own)
    shape = own.shape[:-1]
    both = jnp.stack([even.reshape(*shape, 8, 256), odd.reshape(*shape, 8, 256)], axis=-2)
    return both.reshape(*shape, 4096)


def around(value, axis, index):
    turned = jnp.flip(value, axis)
    return lax.dynamic_slice_in_dim(jnp.concatenate([turned, turned], axis), 7 - index, 8, axis)


AHEAD = [(i, (i + 1) % 8) for i in range(8)]
BACK = [(i, (i + 7) % 8) for i in range(8)]


def hop(value, pairs):
    return lax.ppermute(value, "z", pairs)


def ring(block):
    blocks = [block] + [None] * 7
    for step in range(1, 4):
        blocks[step] = hop(blocks[step - 1], AHEAD)
        blocks[8 - step] = hop(blocks[(9 - step) % 8], BACK)
    fourth = hop(blocks[3][:688], AHEAD), hop(blocks[5][688:], BACK)
    return [*blocks[:4], *blocks[5:]], *fourth


EARLY = (0, 1, 2, 3, 5, 6, 7)


def early_kernel(half, rows, *refs):
    *blocks, out = refs
    total = 0.0
    for j, block in zip(EARLY, blocks):
        total += times(rows[half, :, 256 * j : 256 * j + 256], block[:688])
    out[...] = total


def last_kernel(half, mine, theirs, early_mine, early_theirs, block, out):
    for start, rows, early in ((0, mine, early_mine), (128, theirs, early_theirs)):
        total = early[...] + times(rows[half, :, 1024:1280], block[...])
        out[start : start + 128] = total.astype(out.dtype)


def times(a, b):
    return lax.dot_general(a, b, (((1,), (1,)), ((), ())), preferred_element_type=F32)


VMEM = pl.BlockSpec(memory_space=pltpu.VMEM)


def product(kernel, count, dtype, depth, *operands):
    return pl.pallas_call(
        kernel,
        out_shape=jax.ShapeDtypeStruct((count, 688), dtype),
        in_specs=[VMEM] * len(operands),
        out_specs=VMEM,
        cost_estimate=pl.CostEstimate(flops=2 * count * depth * 688, bytes_accessed=2048 * depth, transcendentals=0),
        compiler_params=pltpu.CompilerParams(vmem_limit_bytes=16 << 20),
    )(*operands)


def early_product(half, rows, blocks):
    kernel = functools.partial(early_kernel, half)
    return product(kernel, 128, F32, 1792, rows, *blocks)


def last_product(half, dtype, *operands):
    kernel = functools.partial(last_kernel, half)
    return product(kernel, 256, dtype, 256, *operands)


def rows_of(core, own, other):
    pieces = []
    for at in range(128 * core, 128 * core + 128, 32):
        pieces += [own[at : at + 32], other[at : at + 32]]
    return jnp.concatenate(pieces, axis=0)


def down_kernel(core, own, other, fourth, *refs):
    *blocks, out = refs
    hidden = rows_of(core, own, other)
    for j in range(8):
        weights = fourth[...] if j == 4 else blocks[j - (j > 4)][688:]
        terms = jnp.dot(hidden, weights, preferred_element_type=F32).astype(out.dtype)
        for x in range(4):
            out[x, j] = terms[64 * x : 64 * x + 64]


def down(core, dtype, own, other, fourth, blocks):
    return pl.pallas_call(
        functools.partial(down_kernel, core),
        out_shape=jax.ShapeDtypeStruct((4, 8, 64, 256), dtype),
        in_specs=[VMEM] * 10,
        out_specs=VMEM,
        cost_estimate=pl.CostEstimate(flops=2 * 256 * 2048 * 344, bytes_accessed=3 << 20, transcendentals=0),
        compiler_params=pltpu.CompilerParams(vmem_limit_bytes=16 << 20),
    )(own, other, fourth, *blocks)


def one_hot(codes):
    return (codes[:, None] == jnp.arange(64, dtype=F32)[None, :].astype(BF16)).astype(BF16)


def program(features, norm_gain, gate_weight, up_weight, down_weight, centroids, list_ids, live):
    yl = lax.axis_index("yl")
    z = lax.axis_index("z")
    weights, last_first, last_second = ring(jnp.concatenate([gate_weight.T, up_weight.T, down_weight], axis=0))

    code = jnp.where(live > 0, list_ids, -1).astype(BF16)
    code_block = jnp.broadcast_to(code[:, None], (8, 128))
    own_x, away_x = (around(v.reshape(8, 8, 256), 1, z).reshape(8, 2048) for v in by_class(features, yl))
    received = swapped(jnp.concatenate([away_x, code_block], axis=1), "yl")
    x = jnp.concatenate([own_x, received[:, :2048]], axis=0)
    other_code = received[:, 2048]
    table, _ = by_class(centroids.astype(BF16), yl)
    sent = jnp.concatenate([x, table.reshape(16, 256)], axis=1)
    copies = jnp.broadcast_to(sent.reshape(2, 1, 8, 2304), (2, 16, 8, 2304))
    mine = lax.all_to_all(copies, ROWS, 1, 1, tiled=True).reshape(2, 128, 2304)
    theirs = swapped(mine, "c")

    early_mine = early_product(1, mine, weights)
    early_theirs = early_product(1, theirs, weights)
    away_part = last_product(1, BF16, mine, theirs, early_mine, early_theirs, last_first)
    away_part = swapped(away_part, "yl")
    early_mine, early_theirs = early_product(0, mine, weights), early_product(0, theirs, weights)
    kept_part = last_product(0, F32, mine, theirs, early_mine, early_theirs, last_first)
    both = kept_part + away_part.astype(F32)
    hidden = (jax.nn.silu(both[:, :344]) * both[:, 344:]).astype(BF16)
    other_hidden = swapped(hidden, "yl")
    to_core = down(1, BF16, hidden, other_hidden, last_second, weights)
    from_core = swapped(to_core, "c")
    terms = down(0, F32, hidden, other_hidden, last_second, weights)
    terms = (terms + from_core.astype(F32)).astype(BF16)

    mine, theirs, terms = lax.optimization_barrier((mine, theirs, terms))
    core = lax.axis_index("c")
    lists = jnp.stack([mine[..., 2048:], theirs[..., 2048:]]).reshape(2, 2, 4, 4, 2048)
    lists = jnp.where(core == 0, lists, lists[::-1])
    lists = lists.transpose(3, 2, 0, 1, 4).reshape(64, 2048)
    picked = jnp.dot(one_hot(code), lists, preferred_element_type=F32).astype(BF16)
    other_picked = jnp.dot(one_hot(other_code), lists, preferred_element_type=F32).astype(BF16)
    coarse = interleaved(picked, swapped(other_picked, "yl"), yl)

    terms = lax.all_to_all(terms, "x", 0, 0, tiled=True)
    terms = jnp.sum(terms.astype(F32), axis=0).astype(BF16)
    terms = terms.reshape(8, 2, 4, 8, 256).transpose(2, 1, 0, 3, 4)
    terms = jnp.where(yl == 0, terms, terms[:, ::-1]).reshape(8, 8, 8, 256)
    terms = lax.all_to_all(terms, ("yh", "yl"), 0, 0, tiled=True)
    terms = jnp.sum(terms.reshape(4, 2, 8, 8, 256).astype(F32), axis=0)
    mixed = around(terms, 1, z).transpose(2, 1, 0, 3).reshape(8, 4096)

    stream = features.astype(F32) + mixed
    scale = lax.rsqrt(jnp.mean(stream * stream, axis=1, keepdims=True) + 1e-05)
    embedding = (stream * scale * norm_gain).astype(BF16)
    alive = (live > 0).astype(F32)[:, None]
    residuals = (alive * (embedding.astype(F32) - coarse.astype(F32))).astype(BF16)

    blocks = embedding.reshape(8, 16, 256).transpose(1, 0, 2)
    blocks = jnp.concatenate([blocks, jnp.broadcast_to(code_block, (16, 8, 128))], axis=2)
    blocks = lax.all_to_all(blocks, SHARD, 0, 0, tiled=True).reshape(128, 384)
    member = one_hot(blocks[:, 256])
    sums = jnp.dot(member.T, blocks[:, :256], preferred_element_type=F32).astype(BF16)
    counts = jnp.sum(member.astype(F32), axis=0).astype(BF16)
    sums = jnp.concatenate([sums, jnp.broadcast_to(counts[:, None], (64, 128))], axis=1)
    sums = lax.all_to_all(sums.reshape(32, 2, 384), LIST, 0, 0, tiled=True)
    sums = jnp.sum(sums.astype(F32), axis=0)
    total = to_everyone(sums[:, :256], SHARD).transpose(1, 0, 2).reshape(2, 4096)
    refreshed = (centroids + total) / (1.0 + sums[:, 256:257])
    return residuals, refreshed


def solution(mesh):
    fine = Mesh(mesh.devices.reshape(4, 4, 2, 8, 2), ("yh", "x", "c", "z", "yl"))
    in_specs = (
        P((*LIST, *SHARD), None),
        P(),
        P(SHARD, LIST),
        P(SHARD, LIST),
        P(LIST, SHARD),
        P(LIST, None),
        P((*LIST, *SHARD)),
        P((*LIST, *SHARD)),
    )
    out_specs = (P((*LIST, *SHARD), None), P(LIST, None))
    return jax.shard_map(program, mesh=fine, in_specs=in_specs, out_specs=out_specs, check_vma=False)
```

```python
import functools

import jax
import jax.numpy as jnp
from jax import lax
from jax.experimental import pallas as pl
from jax.experimental.pallas import tpu as pltpu
from jax.sharding import Mesh, PartitionSpec as P

F32 = jnp.float32
BF16 = jnp.bfloat16
SWAP = [(0, 1), (1, 0)]
ROWS = ("x", "yh")
LIST = ("yh", "x", "c")
SHARD = ("z", "yl")


def swapped(value, axis):
    return lax.ppermute(value, axis, SWAP)


def to_everyone(value, axis):
    copies = jnp.broadcast_to(value, (lax.axis_size(axis), *value.shape))
    return lax.all_to_all(copies, axis, split_axis=0, concat_axis=0, tiled=True)


def by_class(value, mine):
    blocks = value.reshape(*value.shape[:-1], 8, 2, 256)
    even = blocks[..., 0, :].reshape(*value.shape[:-1], 2048)
    odd = blocks[..., 1, :].reshape(*value.shape[:-1], 2048)
    return jnp.where(mine == 0, even, odd), jnp.where(mine == 0, odd, even)


def interleaved(own, other, mine):
    even, odd = jnp.where(mine == 0, own, other), jnp.where(mine == 0, other, own)
    shape = own.shape[:-1]
    both = jnp.stack([even.reshape(*shape, 8, 256), odd.reshape(*shape, 8, 256)], axis=-2)
    return both.reshape(*shape, 4096)


def around(value, axis, index):
    turned = jnp.flip(value, axis)
    return lax.dynamic_slice_in_dim(jnp.concatenate([turned, turned], axis), 7 - index, 8, axis)


AHEAD = [(i, (i + 1) % 8) for i in range(8)]
BACK = [(i, (i + 7) % 8) for i in range(8)]


def hop(value, pairs):
    return lax.ppermute(value, "z", pairs)


def ring(block):
    blocks = [block] + [None] * 7
    for step in range(1, 4):
        blocks[step] = hop(blocks[step - 1], AHEAD)
        blocks[8 - step] = hop(blocks[(9 - step) % 8], BACK)
    fourth = hop(blocks[3][:688], AHEAD), hop(blocks[5][688:], BACK)
    return [*blocks[:4], *blocks[5:]], *fourth


EARLY = (0, 1, 2, 3, 5, 6, 7)


def taken(rows, half, j):
    return rows[:, half, :, 256 * j : 256 * j + 256].reshape(128, 256)


def early_kernel(half, rows, *refs):
    *blocks, out = refs
    total = 0.0
    for j, block in zip(EARLY, blocks):
        total += times(taken(rows, half, j), block[:688])
    out[...] = total


def last_kernel(half, mine, theirs, early_mine, early_theirs, block, out):
    for start, rows, early in ((0, mine, early_mine), (128, theirs, early_theirs)):
        total = early[...] + times(taken(rows, half, 4), block[...])
        out[start : start + 128] = total.astype(out.dtype)


def times(a, b):
    return lax.dot_general(a, b, (((1,), (1,)), ((), ())), preferred_element_type=F32)


VMEM = pl.BlockSpec(memory_space=pltpu.VMEM)


def product(kernel, count, dtype, depth, *operands):
    return pl.pallas_call(
        kernel,
        out_shape=jax.ShapeDtypeStruct((count, 688), dtype),
        in_specs=[VMEM] * len(operands),
        out_specs=VMEM,
        cost_estimate=pl.CostEstimate(flops=2 * count * depth * 688, bytes_accessed=2048 * depth, transcendentals=0),
        compiler_params=pltpu.CompilerParams(vmem_limit_bytes=16 << 20),
    )(*operands)


def early_product(half, rows, blocks):
    kernel = functools.partial(early_kernel, half)
    return product(kernel, 128, F32, 1792, rows, *blocks)


def last_product(half, dtype, *operands):
    kernel = functools.partial(last_kernel, half)
    return product(kernel, 256, dtype, 256, *operands)


def rows_of(core, own, other):
    pieces = []
    for at in range(128 * core, 128 * core + 128, 32):
        pieces += [own[at : at + 32], other[at : at + 32]]
    return jnp.concatenate(pieces, axis=0)


def down_kernel(core, own, other, fourth, *refs):
    *blocks, out = refs
    hidden = rows_of(core, own, other)
    for j in range(8):
        weights = fourth[...] if j == 4 else blocks[j - (j > 4)][688:]
        terms = jnp.dot(hidden, weights, preferred_element_type=F32).astype(out.dtype)
        for x in range(4):
            out[x, j] = terms[64 * x : 64 * x + 64]


def down(core, dtype, own, other, fourth, blocks):
    return pl.pallas_call(
        functools.partial(down_kernel, core),
        out_shape=jax.ShapeDtypeStruct((4, 8, 64, 256), dtype),
        in_specs=[VMEM] * 10,
        out_specs=VMEM,
        cost_estimate=pl.CostEstimate(flops=2 * 256 * 2048 * 344, bytes_accessed=3 << 20, transcendentals=0),
        compiler_params=pltpu.CompilerParams(vmem_limit_bytes=16 << 20),
    )(own, other, fourth, *blocks)


def one_hot(codes):
    return (codes[:, None] == jnp.arange(64, dtype=F32)[None, :].astype(BF16)).astype(BF16)


def program(features, norm_gain, gate_weight, up_weight, down_weight, centroids, list_ids, live):
    yl = lax.axis_index("yl")
    z = lax.axis_index("z")
    weights, last_first, last_second = ring(jnp.concatenate([gate_weight.T, up_weight.T, down_weight], axis=0))

    code = jnp.where(live > 0, list_ids, -1).astype(BF16)
    code_block = jnp.broadcast_to(code[:, None], (8, 128))
    own_x, away_x = (around(v.reshape(8, 8, 256), 1, z).reshape(8, 2048) for v in by_class(features, yl))
    received = swapped(jnp.concatenate([away_x, code_block], axis=1), "yl")
    x = jnp.concatenate([own_x, received[:, :2048]], axis=0)
    other_code = received[:, 2048]
    table, _ = by_class(centroids.astype(BF16), yl)
    sent = jnp.concatenate([x, table.reshape(16, 256)], axis=1)
    mine = to_everyone(sent.reshape(2, 8, 2304), ROWS)
    theirs = swapped(mine, "c")

    early_mine = early_product(1, mine, weights)
    early_theirs = early_product(1, theirs, weights)
    away_part = last_product(1, BF16, mine, theirs, early_mine, early_theirs, last_first)
    away_part = swapped(away_part, "yl")
    early_mine, early_theirs = early_product(0, mine, weights), early_product(0, theirs, weights)
    kept_part = last_product(0, F32, mine, theirs, early_mine, early_theirs, last_first)
    both = kept_part + away_part.astype(F32)
    hidden = (jax.nn.silu(both[:, :344]) * both[:, 344:]).astype(BF16)
    other_hidden = swapped(hidden, "yl")
    to_core = down(1, BF16, hidden, other_hidden, last_second, weights)
    from_core = swapped(to_core, "c")
    terms = down(0, F32, hidden, other_hidden, last_second, weights)
    terms = (terms + from_core.astype(F32)).astype(BF16)

    mine, theirs, terms = lax.optimization_barrier((mine, theirs, terms))
    core = lax.axis_index("c")
    lists = jnp.stack([mine[..., 2048:], theirs[..., 2048:]]).reshape(2, 4, 4, 2, 2048)
    lists = jnp.where(core == 0, lists, lists[::-1])
    lists = lists.transpose(2, 1, 0, 3, 4).reshape(64, 2048)
    picked = jnp.dot(one_hot(code), lists, preferred_element_type=F32).astype(BF16)
    other_picked = jnp.dot(one_hot(other_code), lists, preferred_element_type=F32).astype(BF16)
    coarse = interleaved(picked, swapped(other_picked, "yl"), yl)

    terms = lax.all_to_all(terms, "x", 0, 0, tiled=True)
    terms = jnp.sum(terms.astype(F32), axis=0).astype(BF16)
    terms = terms.reshape(8, 2, 4, 8, 256).transpose(2, 1, 0, 3, 4)
    terms = jnp.where(yl == 0, terms, terms[:, ::-1]).reshape(8, 8, 8, 256)
    terms = lax.all_to_all(terms, ("yh", "yl"), 0, 0, tiled=True)
    terms = jnp.sum(terms.reshape(4, 2, 8, 8, 256).astype(F32), axis=0)
    mixed = around(terms, 1, z).transpose(2, 1, 0, 3).reshape(8, 4096)

    stream = features.astype(F32) + mixed
    scale = lax.rsqrt(jnp.mean(stream * stream, axis=1, keepdims=True) + 1e-05)
    embedding = (stream * scale * norm_gain).astype(BF16)
    alive = (live > 0).astype(F32)[:, None]
    residuals = (alive * (embedding.astype(F32) - coarse.astype(F32))).astype(BF16)

    blocks = embedding.reshape(8, 16, 256).transpose(1, 0, 2)
    blocks = jnp.concatenate([blocks, jnp.broadcast_to(code_block, (16, 8, 128))], axis=2)
    blocks = lax.all_to_all(blocks, SHARD, 0, 0, tiled=True).reshape(128, 384)
    member = one_hot(blocks[:, 256])
    sums = jnp.dot(member.T, blocks[:, :256], preferred_element_type=F32).astype(BF16)
    counts = jnp.sum(member.astype(F32), axis=0).astype(BF16)
    sums = jnp.concatenate([sums, jnp.broadcast_to(counts[:, None], (64, 128))], axis=1)
    sums = lax.all_to_all(sums.reshape(32, 2, 384), LIST, 0, 0, tiled=True)
    sums = jnp.sum(sums.astype(F32), axis=0)
    total = to_everyone(sums[:, :256], SHARD).transpose(1, 0, 2).reshape(2, 4096)
    refreshed = (centroids + total) / (1.0 + sums[:, 256:257])
    return residuals, refreshed


def solution(mesh):
    fine = Mesh(mesh.devices.reshape(4, 4, 2, 8, 2), ("yh", "x", "c", "z", "yl"))
    in_specs = (
        P((*LIST, *SHARD), None),
        P(),
        P(SHARD, LIST),
        P(SHARD, LIST),
        P(LIST, SHARD),
        P(LIST, None),
        P((*LIST, *SHARD)),
        P((*LIST, *SHARD)),
    )
    out_specs = (P((*LIST, *SHARD), None), P(LIST, None))
    return jax.shard_map(program, mesh=fine, in_specs=in_specs, out_specs=out_specs, check_vma=False)
```

```python
import functools

import jax
import jax.numpy as jnp
from jax import lax
from jax.experimental import pallas as pl
from jax.experimental.pallas import tpu as pltpu
from jax.sharding import Mesh, PartitionSpec as P

F32 = jnp.float32
BF16 = jnp.bfloat16
SWAP = [(0, 1), (1, 0)]
ROWS = ("x", "yh")
LIST = ("yh", "x", "c")
SHARD = ("z", "yl")


def swapped(value, axis):
    return lax.ppermute(value, axis, SWAP)


def to_everyone(value, axis):
    copies = jnp.broadcast_to(value, (lax.axis_size(axis), *value.shape))
    return lax.all_to_all(copies, axis, split_axis=0, concat_axis=0, tiled=True)


def by_class(value, mine):
    blocks = value.reshape(*value.shape[:-1], 8, 2, 256)
    even = blocks[..., 0, :].reshape(*value.shape[:-1], 2048)
    odd = blocks[..., 1, :].reshape(*value.shape[:-1], 2048)
    return jnp.where(mine == 0, even, odd), jnp.where(mine == 0, odd, even)


def interleaved(own, other, mine):
    even, odd = jnp.where(mine == 0, own, other), jnp.where(mine == 0, other, own)
    shape = own.shape[:-1]
    both = jnp.stack([even.reshape(*shape, 8, 256), odd.reshape(*shape, 8, 256)], axis=-2)
    return both.reshape(*shape, 4096)


def around(value, axis, index):
    turned = jnp.flip(value, axis)
    return lax.dynamic_slice_in_dim(jnp.concatenate([turned, turned], axis), 7 - index, 8, axis)


AHEAD = [(i, (i + 1) % 8) for i in range(8)]
BACK = [(i, (i + 7) % 8) for i in range(8)]


def hop(value, pairs):
    return lax.ppermute(value, "z", pairs)


def ring(block):
    blocks = [block] + [None] * 7
    for step in range(1, 4):
        blocks[step] = hop(blocks[step - 1], AHEAD)
        blocks[8 - step] = hop(blocks[(9 - step) % 8], BACK)
    fourth = hop(blocks[3][:688], AHEAD), hop(blocks[5][688:], BACK)
    return [*blocks[:4], *blocks[5:]], *fourth


EARLY = (0, 1, 2, 3, 5, 6, 7)


def taken(rows, half, j):
    return rows[:, half, :, 256 * j : 256 * j + 256].reshape(128, 256)


def early_kernel(half, rows, *refs):
    *blocks, out = refs
    total = 0.0
    for j, block in zip(EARLY, blocks):
        total += times(taken(rows, half, j), block[:688])
    out[...] = total


def last_kernel(half, mine, theirs, early_mine, early_theirs, block, out):
    for start, rows, early in ((0, mine, early_mine), (128, theirs, early_theirs)):
        total = early[...] + times(taken(rows, half, 4), block[...])
        out[start : start + 128] = total.astype(out.dtype)


def times(a, b):
    return lax.dot_general(a, b, (((1,), (1,)), ((), ())), preferred_element_type=F32)


VMEM = pl.BlockSpec(memory_space=pltpu.VMEM)


def product(kernel, count, dtype, depth, *operands):
    return pl.pallas_call(
        kernel,
        out_shape=jax.ShapeDtypeStruct((count, 688), dtype),
        in_specs=[VMEM] * len(operands),
        out_specs=VMEM,
        cost_estimate=pl.CostEstimate(flops=2 * count * depth * 688, bytes_accessed=2048 * depth, transcendentals=0),
        compiler_params=pltpu.CompilerParams(vmem_limit_bytes=16 << 20),
    )(*operands)


def early_product(half, rows, blocks):
    kernel = functools.partial(early_kernel, half)
    return product(kernel, 128, F32, 1792, rows, *blocks)


def last_product(half, dtype, *operands):
    kernel = functools.partial(last_kernel, half)
    return product(kernel, 256, dtype, 256, *operands)


def rows_of(core, own, other):
    pieces = []
    for at in range(128 * core, 128 * core + 128, 32):
        pieces += [own[at : at + 32], other[at : at + 32]]
    return jnp.concatenate(pieces, axis=0)


def down_kernel(core, own, other, fourth, *refs):
    *blocks, out = refs
    hidden = rows_of(core, own, other)
    for j in range(8):
        weights = fourth[...] if j == 4 else blocks[j - (j > 4)][688:]
        terms = jnp.dot(hidden, weights, preferred_element_type=F32).astype(out.dtype)
        for x in range(4):
            out[x, j] = terms[64 * x : 64 * x + 64]


def down(core, dtype, own, other, fourth, blocks):
    return pl.pallas_call(
        functools.partial(down_kernel, core),
        out_shape=jax.ShapeDtypeStruct((4, 8, 64, 256), dtype),
        in_specs=[VMEM] * 10,
        out_specs=VMEM,
        cost_estimate=pl.CostEstimate(flops=2 * 256 * 2048 * 344, bytes_accessed=3 << 20, transcendentals=0),
        compiler_params=pltpu.CompilerParams(vmem_limit_bytes=16 << 20),
    )(own, other, fourth, *blocks)


def one_hot(codes):
    return (codes[:, None] == jnp.arange(64, dtype=F32)[None, :].astype(BF16)).astype(BF16)


def program(features, norm_gain, gate_weight, up_weight, down_weight, centroids, list_ids, live):
    yl = lax.axis_index("yl")
    z = lax.axis_index("z")
    weights, last_first, last_second = ring(jnp.concatenate([gate_weight.T, up_weight.T, down_weight], axis=0))

    code = jnp.where(live > 0, list_ids, -1).astype(BF16)
    code_block = jnp.broadcast_to(code[:, None], (8, 128))
    own_x, away_x = (around(v.reshape(8, 8, 256), 1, z).reshape(8, 2048) for v in by_class(features, yl))
    received = swapped(jnp.concatenate([away_x, code_block], axis=1), "yl")
    x = jnp.concatenate([own_x, received[:, :2048]], axis=0)
    other_code = received[:, 2048]
    table, _ = by_class(centroids.astype(BF16), yl)
    sent = jnp.concatenate([x, table.reshape(16, 256)], axis=1)
    mine = to_everyone(sent.reshape(2, 8, 2304), ROWS)
    theirs = swapped(mine, "c")

    early_mine = early_product(1, mine, weights)
    early_theirs = early_product(1, theirs, weights)
    away_part = last_product(1, BF16, mine, theirs, early_mine, early_theirs, last_first)
    away_part = swapped(away_part, "yl")
    early_mine, early_theirs = early_product(0, mine, weights), early_product(0, theirs, weights)
    kept_part = last_product(0, F32, mine, theirs, early_mine, early_theirs, last_first)
    both = kept_part + away_part.astype(F32)
    hidden = (jax.nn.silu(both[:, :344]) * both[:, 344:]).astype(BF16)
    other_hidden = swapped(hidden, "yl")
    to_core = down(1, BF16, hidden, other_hidden, last_second, weights)
    from_core = swapped(to_core, "c")
    terms = down(0, F32, hidden, other_hidden, last_second, weights)
    terms = (terms + from_core.astype(F32)).astype(BF16)

    mine, theirs, terms = lax.optimization_barrier((mine, theirs, terms))
    core = lax.axis_index("c")
    lists = jnp.stack([mine[..., 2048:], theirs[..., 2048:]]).reshape(2, 4, 4, 2, 2048)
    lists = jnp.where(core == 0, lists, lists[::-1])
    lists = lists.transpose(2, 1, 0, 3, 4).reshape(64, 2048)
    picked = jnp.dot(one_hot(code), lists, preferred_element_type=F32).astype(BF16)
    other_picked = jnp.dot(one_hot(other_code), lists, preferred_element_type=F32).astype(BF16)
    coarse = interleaved(picked, swapped(other_picked, "yl"), yl)

    terms = lax.all_to_all(terms, "x", 0, 0, tiled=True)
    terms = jnp.sum(terms.astype(F32), axis=0).astype(BF16)
    terms = terms.reshape(8, 2, 4, 8, 256).transpose(2, 1, 0, 3, 4)
    terms = jnp.where(yl == 0, terms, terms[:, ::-1]).reshape(8, 8, 8, 256)
    terms = lax.all_to_all(terms, ("yh", "yl"), 0, 0, tiled=True)
    terms = jnp.sum(terms.reshape(4, 2, 8, 8, 256).astype(F32), axis=0)
    mixed = around(terms, 1, z).transpose(2, 1, 0, 3).reshape(8, 4096)

    stream = features.astype(F32) + mixed
    scale = lax.rsqrt(jnp.mean(stream * stream, axis=1, keepdims=True) + 1e-05)
    embedding = (stream * scale * norm_gain).astype(BF16)
    alive = (live > 0).astype(F32)[:, None]
    residuals = (alive * (embedding.astype(F32) - coarse.astype(F32))).astype(BF16)

    blocks = embedding.reshape(8, 8, 512).transpose(1, 0, 2)
    blocks = jnp.concatenate([blocks, jnp.broadcast_to(code_block, (8, 8, 128))], axis=2)
    blocks = lax.all_to_all(blocks, "z", 0, 0, tiled=True).reshape(64, 640)
    member = one_hot(blocks[:, 512])
    sums = jnp.dot(member.T, blocks[:, :512], preferred_element_type=F32).astype(BF16)
    counts = jnp.sum(member.astype(F32), axis=0).astype(BF16)
    sums = jnp.concatenate([sums, jnp.broadcast_to(counts[:, None], (64, 128))], axis=1)
    sums = lax.all_to_all(sums.reshape(32, 2, 640), LIST, 0, 0, tiled=True)
    sums = jnp.sum(sums.astype(F32), axis=0)
    sums = to_everyone(sums, SHARD).reshape(8, 2, 2, 640).sum(axis=1)
    total = sums[:, :, :512].transpose(1, 0, 2).reshape(2, 4096)
    refreshed = (centroids + total) / (1.0 + sums[0, :, 512:513])
    return residuals, refreshed


def solution(mesh):
    fine = Mesh(mesh.devices.reshape(4, 4, 2, 8, 2), ("yh", "x", "c", "z", "yl"))
    in_specs = (
        P((*LIST, *SHARD), None),
        P(),
        P(SHARD, LIST),
        P(SHARD, LIST),
        P(LIST, SHARD),
        P(LIST, None),
        P((*LIST, *SHARD)),
        P((*LIST, *SHARD)),
    )
    out_specs = (P((*LIST, *SHARD), None), P(LIST, None))
    return jax.shard_map(program, mesh=fine, in_specs=in_specs, out_specs=out_specs, check_vma=False)
```
